32 devices in a mesh: sweep: 1, dp: 8 (over z, y), tensor: 4 (over x, core).
Axes of the slice: x: 2, y: 2, z: 4, core: 2. Of those that a mesh axis runs over, the one named last changes fastest.
Arguments:
- checkpoint: bfloat16 [1024, 8192], P(('sweep', 'dp'), 'tensor'), may hold values from -6 to 6
- norm_gain: bfloat16 [8192], P(('sweep', 'tensor')), may hold values from 0.5 to 1.5
- w_query: bfloat16 [8192, 4096], P(('sweep', 'dp'), 'tensor'), may hold values from -1 to 1
- w_key: bfloat16 [8192, 512], P(('sweep', 'dp'), 'tensor'), may hold values from -8 to 8
- w_value: bfloat16 [8192, 512], P(('sweep', 'dp'), 'tensor'), may hold values from -0.0625 to 0.0625
- grad_attn: bfloat16 [1024, 4096], P(('sweep', 'dp'), 'tensor'), may hold values from -6 to 6
Outputs:
- d_checkpoint: bfloat16 [1024, 8192], P(('sweep', 'dp'), 'tensor')
- grad_gain: float32 [8192], P(('sweep', 'tensor'))
- grad_query: float32 [8192, 4096], P(('sweep', 'dp'), 'tensor')
- grad_key: float32 [8192, 512], P(('sweep', 'dp'), 'tensor')
- grad_value: float32 [8192, 512], P(('sweep', 'dp'), 'tensor')
The draws below stay inside these ranges and needn't reach their ends.
All inputs are finite; a program needn't handle non-finite values.
Results may differ from the reference program's by a relative error of at most 0.025.
The reference program's roundings to bfloat16 on the way count: a program that leaves them out, or rounds other values in their place, can miss the bound.
Values may be sent and summed in bfloat16 or wider, within the bound.
A program may use at most 128 MiB of HBM per device.

```python
import jax
import jax.numpy as jnp
from jax import lax

D = 8192
QHEADS = 32
KVHEADS = 4
HD = 128
TOK_DEV = 128
SEQ = 1024
N_DP = 8
N_TENSOR = 4


def query_matrix(key):
    anchor = jax.random.fold_in(key, 11)
    return jax.random.truncated_normal(anchor, -4.0, 4.0, (D, QHEADS * HD), jnp.float32) * D ** (-0.5)


def draw_w_query(key, part):
    return query_matrix(key).astype(jnp.bfloat16)


def draw_w_key(key, part):
    noise = jax.random.truncated_normal(jax.random.fold_in(key, 23), -4.0, 4.0, (D, KVHEADS * HD), jnp.float32) * D ** (-0.5)
    return noise.astype(jnp.bfloat16)


def steps_of(key, shape, split, low, high):
    def one(axis_at, shards_of):
        heights = jax.random.uniform(jax.random.fold_in(jax.random.fold_in(key, 6), axis_at), (shards_of,), jnp.float32, low / len(split), high / len(split))
        return jnp.repeat(jnp.exp(heights), shape[axis_at] // shards_of).reshape((-1,) + (1,) * (len(shape) - axis_at - 1))

    level = one(*split[0])
    for cut in split[1:]:
        level = level * one(*cut)
    return level


def gaussian(stream_key, dims, scale, most, cuts=(), kind=jnp.bfloat16):
    loudness = steps_of(stream_key, dims, cuts, -0.22, 0.18) if cuts else 1.0
    drawn = jax.random.normal(stream_key, dims, jnp.float32) * scale * loudness
    return jnp.minimum(jnp.maximum(drawn, -most), most).astype(kind)


def setup_inputs(seed: int = 0, part: int = 0) -> dict:
    streams_of = jax.random.split(jax.random.key(seed), 7)
    own_keys = jax.random.split(jax.random.fold_in(streams_of[6], part), 7)
    return {
        "checkpoint": gaussian(own_keys[0], (SEQ, D), 1.0, 6.0, ((0, 8), (1, 4))),
        "norm_gain": jnp.clip(1.0 + 0.1 * jax.random.normal(own_keys[1], (D,), jnp.float32), 0.5, 1.5).astype(jnp.bfloat16),
        "w_query": draw_w_query(jax.random.fold_in(jax.random.fold_in(streams_of[6], part), 71), part),
        "w_key": draw_w_key(jax.random.fold_in(jax.random.fold_in(streams_of[6], part), 71), part),
        "w_value": gaussian(own_keys[4], (D, KVHEADS * HD), D ** -0.5, 0.0625, ((0, 8), (1, 4))),
        "grad_attn": gaussian(own_keys[5], (SEQ, QHEADS * HD), 1.0, 6.0, ((0, 8), (1, 4))),
    }


EPS = 1e-05
THETA = 500000.0

def round_half(field):
    return lax.optimization_barrier(field.astype(jnp.bfloat16))

def angles(positions, head_width):
    frequency = THETA ** (-(jnp.arange(head_width // 2, dtype=jnp.float32) * 2.0) / head_width)
    turned = positions.astype(jnp.float32)[:, None] * frequency[None, :]
    return (jnp.cos(turned)[:, None, :], jnp.sin(turned)[:, None, :])

def rotate(field, cosine_table, sine_table):
    half_width = field.shape[-1] // 2
    front_half = field[..., :half_width]
    back_half = field[..., half_width:]
    return jnp.concatenate([front_half * cosine_table - back_half * sine_table, back_half * cosine_table + front_half * sine_table], -1)

def rotate_back(field, cosine_table, sine_table):
    half_width = field.shape[-1] // 2
    front_half = field[..., :half_width]
    back_half = field[..., half_width:]
    return jnp.concatenate([front_half * cosine_table + back_half * sine_table, back_half * cosine_table - front_half * sine_table], -1)

def reference(checkpoint, norm_gain, w_query, w_key, w_value, grad_attn):
    x_wide = checkpoint.astype(jnp.float32)
    gain_wide = norm_gain.astype(jnp.float32)
    inverse = lax.rsqrt(lax.optimization_barrier(jnp.mean(x_wide * x_wide, -1, keepdims=True)) + EPS)
    normed = (x_wide * inverse * gain_wide).astype(jnp.bfloat16)
    queries = jnp.dot(normed, w_query, preferred_element_type=jnp.float32).reshape(SEQ, QHEADS, HD)
    keyed = jnp.transpose(jnp.dot(normed, w_key, preferred_element_type=jnp.float32).reshape(SEQ, HD, KVHEADS), (0, 2, 1))
    valued = jnp.transpose(jnp.dot(normed, w_value, preferred_element_type=jnp.float32).reshape(SEQ, HD, KVHEADS), (0, 2, 1))
    cosine_table, sine_table = angles(jnp.arange(SEQ, dtype=jnp.int32), HD)
    query_rot = rotate(queries, cosine_table, sine_table).astype(jnp.bfloat16)
    key_rot = rotate(keyed, cosine_table, sine_table).astype(jnp.bfloat16)
    value_half = valued.astype(jnp.bfloat16)
    group_size = QHEADS // KVHEADS
    run_heads = min(QHEADS // N_TENSOR, group_size)
    run_count = group_size // run_heads
    score_scale = HD ** (-0.5)
    key_wide = key_rot.astype(jnp.float32)
    value_wide = value_half.astype(jnp.float32)
    upstream_all = grad_attn.reshape(SEQ, KVHEADS, group_size, HD)
    query_all = query_rot.reshape(SEQ, KVHEADS, group_size, HD)

    def attend_block(block_index):
        first_row = (block_index * TOK_DEV).astype(jnp.int32)
        query_grp = lax.dynamic_slice_in_dim(query_all, first_row, TOK_DEV, 0).astype(jnp.float32)
        upstream = lax.dynamic_slice_in_dim(upstream_all, first_row, TOK_DEV, 0).astype(jnp.float32)
        scores = jnp.einsum('tkgd,skd->kgts', query_grp, key_wide) * score_scale
        allowed = (first_row + jnp.arange(TOK_DEV, dtype=jnp.int32))[:, None] >= jnp.arange(SEQ, dtype=jnp.int32)[None, :]
        scores = jnp.where(allowed, scores, -jnp.inf)
        row_top = lax.optimization_barrier(jnp.max(scores, -1, keepdims=True))
        raw_weights = jnp.exp(scores - row_top)
        chances = raw_weights / lax.optimization_barrier(jnp.sum(raw_weights, -1, keepdims=True))
        chances_half = round_half(chances).astype(jnp.float32)
        attended = jnp.einsum('kgts,skd->tkgd', chances_half, value_wide)
        row_delta = lax.optimization_barrier(jnp.sum(upstream * attended, -1))
        prob_grads = jnp.einsum('tkgd,skd->kgts', upstream, value_wide)
        dscore = chances * (prob_grads - jnp.transpose(row_delta, (1, 2, 0))[..., None])
        dscore_half = round_half(dscore).astype(jnp.float32)
        dquery = jnp.einsum('kgts,skd->tkgd', dscore_half, key_wide) * score_scale
        dscore_runs = dscore_half.reshape(KVHEADS, run_count, run_heads, TOK_DEV, SEQ)
        chances_runs = chances_half.reshape(KVHEADS, run_count, run_heads, TOK_DEV, SEQ)
        query_runs = query_grp.reshape(TOK_DEV, KVHEADS, run_count, run_heads, HD)
        upstream_runs = upstream.reshape(TOK_DEV, KVHEADS, run_count, run_heads, HD)
        dkey_part = jnp.einsum('krgts,tkrgd->skrd', dscore_runs, query_runs) * score_scale
        dvalue_part = jnp.einsum('krgts,tkrgd->skrd', chances_runs, upstream_runs)
        return (dquery.reshape(TOK_DEV, QHEADS, HD), dkey_part.astype(jnp.bfloat16), dvalue_part.astype(jnp.bfloat16))
    dquery_all, dkey_parts, dvalue_parts = lax.map(attend_block, jnp.arange(N_DP, dtype=jnp.int32))
    dquery_all = dquery_all.reshape(SEQ, QHEADS, HD)
    dkey_sum = lax.optimization_barrier(jnp.sum(dkey_parts.astype(jnp.float32), (0, 3)))
    dvalue_sum = lax.optimization_barrier(jnp.sum(dvalue_parts.astype(jnp.float32), (0, 3)))
    dquery_pre = rotate_back(dquery_all, cosine_table, sine_table).astype(jnp.bfloat16).reshape(SEQ, QHEADS * HD)
    dkey_pre = jnp.transpose(rotate_back(dkey_sum, cosine_table, sine_table).astype(jnp.bfloat16), (0, 2, 1)).reshape(SEQ, KVHEADS * HD)
    dvalue_pre = jnp.transpose(dvalue_sum.astype(jnp.bfloat16), (0, 2, 1)).reshape(SEQ, KVHEADS * HD)
    per_query = QHEADS * HD // N_TENSOR
    per_key = KVHEADS * HD // N_TENSOR
    dnormed = jnp.zeros((SEQ, D), jnp.float32)
    for member in range(N_TENSOR):
        query_cols = slice(member * per_query, (member + 1) * per_query)
        key_cols = slice(member * per_key, (member + 1) * per_key)
        partial_term = jnp.dot(dquery_pre[:, query_cols], w_query[:, query_cols].T, preferred_element_type=jnp.float32)
        partial_term = partial_term + jnp.dot(dkey_pre[:, key_cols], w_key[:, key_cols].T, preferred_element_type=jnp.float32)
        partial_term = partial_term + jnp.dot(dvalue_pre[:, key_cols], w_value[:, key_cols].T, preferred_element_type=jnp.float32)
        dnormed = dnormed + round_half(partial_term).astype(jnp.float32)
    grad_gain = lax.optimization_barrier(jnp.sum(dnormed * x_wide * inverse, 0))
    row_sum = lax.optimization_barrier(jnp.sum(gain_wide * dnormed * x_wide, -1, keepdims=True))
    d_checkpoint = (inverse * gain_wide * dnormed - x_wide * inverse ** 3 * row_sum / D).astype(jnp.bfloat16)
    token_grads = jnp.concatenate([dquery_pre, dkey_pre, dvalue_pre], 1)

    def add_rows(running, block_index):
        first_row = (block_index * TOK_DEV).astype(jnp.int32)
        block_x = lax.dynamic_slice_in_dim(normed, first_row, TOK_DEV, 0)
        block_g = lax.dynamic_slice_in_dim(token_grads, first_row, TOK_DEV, 0)
        term = jnp.dot(block_x.T, block_g, preferred_element_type=jnp.float32)
        return (running + round_half(term).astype(jnp.float32), None)
    grads_all, unused = lax.scan(add_rows, jnp.zeros((D, (QHEADS + 2 * KVHEADS) * HD), jnp.float32), jnp.arange(N_DP, dtype=jnp.int32))
    query_width = QHEADS * HD
    key_width = KVHEADS * HD
    grad_query = grads_all[:, :query_width]
    grad_key = grads_all[:, query_width:query_width + key_width]
    grad_value = grads_all[:, query_width + key_width:]
    return (d_checkpoint, grad_gain, grad_query, grad_key, grad_value)
```

```python
import functools

import jax
import jax.numpy as jnp
from jax import lax
from jax.experimental import pallas as pl
from jax.experimental.pallas import tpu as pltpu
from jax.sharding import PartitionSpec as P

QHEADS = 32
KVHEADS = 4
HD = 128
EPS = 1e-05
THETA = 500000.0
PAD = 16
MESH = pl.DeviceIdType.MESH
VMEM = pltpu.VMEM


def copy_to(src, dst, send_sem, recv_sem, dp, tensor):
    return pltpu.make_async_remote_copy(
        src_ref=src,
        dst_ref=dst,
        send_sem=send_sem,
        recv_sem=recv_sem,
        device_id={"dp": dp, "tensor": tensor},
        device_id_type=MESH,
    )


def where_am_i():
    return lax.axis_index("dp"), lax.axis_index("tensor")


def meet(ndp, nt):
    dp, tn = where_am_i()
    me, count = dp * nt + tn, ndp * nt
    barrier = pltpu.get_barrier_semaphore()
    for k in range(1, count):
        other = lax.rem(me + k, count)
        pl.semaphore_signal(
            barrier,
            inc=1,
            device_id={"dp": other // nt, "tensor": lax.rem(other, nt)},
            device_id_type=MESH,
        )
    pl.semaphore_wait(barrier, count - 1)


class Sends:
    def __init__(self, sems):
        self.sems, self.used, self.waits = sems, 0, []

    def go(self, src, dst, recv_sem, dp, tensor):
        copy = copy_to(src, dst, self.sems.at[self.used], recv_sem, dp, tensor)
        self.used += 1
        copy.start()
        self.waits.append(copy)

    def finish(self):
        for copy in self.waits:
            copy.wait_send()


def to_everyone(sends, ndp, nt, source, target, recv):
    dp, tn = where_am_i()
    me, count = dp * nt + tn, ndp * nt
    for k in range(1, count):
        other = lax.rem(me + k, count)
        odp, otn = other // nt, lax.rem(other, nt)
        sends.go(source(odp, otn), target, recv.at[me], odp, otn)


def from_everyone(ndp, nt, slot, recv, send_sem):
    dp, tn = where_am_i()
    me, count = dp * nt + tn, ndp * nt
    for k in range(1, count):
        other = lax.rem(me + count - k, count)
        odp, otn = other // nt, lax.rem(other, nt)
        copy_to(slot(odp, otn), slot(odp, otn), send_sem, recv.at[other], odp, otn).wait_recv()


def gather_start(sends, ndp, source, out, recv):
    dp, tn = where_am_i()
    outer, inner, no = dp // 2, lax.rem(dp, 2), ndp // 2
    for k in range(1, no):
        sends.go(source, out.at[dp], recv.at[dp], lax.rem(outer + k, no) * 2 + inner, tn)
    sends.go(source, out.at[dp], recv.at[dp], outer * 2 + 1 - inner, tn)


def gather_finish(sends, ndp, out, recv):
    dp, tn = where_am_i()
    outer, inner, no = dp // 2, lax.rem(dp, 2), ndp // 2
    partner = outer * 2 + 1 - inner
    for k in range(1, no):
        slot = lax.rem(outer + no - k, no) * 2 + inner
        copy_to(out.at[slot], out.at[slot], sends.sems.at[0], recv.at[slot], slot, tn).wait_recv()
        sends.go(out.at[slot], out.at[slot], recv.at[slot], partner, tn)
    for k in range(no):
        slot = lax.rem(outer + no - k, no) * 2 + 1 - inner
        copy_to(out.at[slot], out.at[slot], sends.sems.at[0], recv.at[slot], partner, tn).wait_recv()


def swap_dp(sends, ndp, source, out, recv):
    dp, tn = where_am_i()
    for k in range(1, ndp):
        other = lax.rem(dp + k, ndp)
        sends.go(source.at[other], out.at[dp], recv.at[dp], other, tn)


def swap_dp_finish(sends, ndp, out, recv):
    dp, tn = where_am_i()
    for k in range(1, ndp):
        other = lax.rem(dp + ndp - k, ndp)
        copy_to(out.at[other], out.at[other], sends.sems.at[0], recv.at[other], other, tn).wait_recv()


def spread_kernel(ndp, nt, x_ref, ss_ref, x_out, ss_out, local, ssem, xrecv, srecv):
    dp, tn = where_am_i()
    per = ndp // nt
    meet(ndp, nt)
    sends = Sends(ssem)
    own = pltpu.make_async_copy(ss_ref, ss_out.at[dp, tn], local.at[0])
    own.start()
    firsts = []
    for s in range(per):
        target, relay = tn * per + s, lax.rem(dp, nt)
        mine = jnp.logical_and(target == dp, relay == tn)
        copy = copy_to(x_ref.at[s], x_out.at[dp], ssem.at[sends.used], xrecv.at[dp], target, relay)
        sends.used += 1
        here = pltpu.make_async_copy(x_ref.at[s], x_out.at[dp], local.at[1])

        @pl.when(mine)
        def _():
            here.start()
            here.wait()

        @pl.when(jnp.logical_not(mine))
        def _():
            copy.start()

        firsts.append((mine, copy))
    to_everyone(sends, ndp, nt, lambda a, b: ss_ref, ss_out.at[dp, tn], srecv)
    outer, inner, no = tn // 2, lax.rem(tn, 2), nt // 2
    partner = outer * 2 + 1 - inner
    for m in range(per):
        slot = m * nt + tn
        block = x_out.at[slot]
        mine = jnp.logical_and(slot == dp, dp // per == tn)

        @pl.when(jnp.logical_not(mine))
        def _():
            copy_to(block, block, ssem.at[0], xrecv.at[slot], slot, dp // per).wait_recv()

        for k in range(1, no):
            sends.go(block, block, xrecv.at[slot], dp, lax.rem(outer + k, no) * 2 + inner)
        sends.go(block, block, xrecv.at[slot], dp, partner)
    for k in range(1, no):
        for m in range(per):
            slot = m * nt + lax.rem(outer + no - k, no) * 2 + inner
            block = x_out.at[slot]
            copy_to(block, block, ssem.at[0], xrecv.at[slot], dp, partner).wait_recv()
            sends.go(block, block, xrecv.at[slot], dp, partner)
    for k in range(no):
        for m in range(per):
            slot = m * nt + lax.rem(outer + no - k, no) * 2 + 1 - inner
            block = x_out.at[slot]
            copy_to(block, block, ssem.at[0], xrecv.at[slot], dp, partner).wait_recv()
    from_everyone(ndp, nt, lambda a, b: ss_out.at[a, b], srecv, ssem.at[0])
    own.wait()
    for mine, copy in firsts:

        @pl.when(jnp.logical_not(mine))
        def _():
            copy.wait_send()

    sends.finish()


def forward_kernel(ndp, nt, q_ref, kv_ref, q_out, kv_out, local, ssem, qrecv, kvrecv):
    dp, tn = where_am_i()
    meet(ndp, nt)
    sends = Sends(ssem)
    kv_own = pltpu.make_async_copy(kv_ref.at[tn * KVHEADS // nt, dp], kv_out.at[dp, tn], local.at[0])
    q_own = pltpu.make_async_copy(q_ref.at[dp], q_out.at[dp], local.at[1])
    kv_own.start()
    q_own.start()
    to_everyone(
        sends, ndp, nt, lambda a, b: kv_ref.at[b * KVHEADS // nt, a], kv_out.at[dp, tn], kvrecv
    )
    swap_dp(sends, ndp, q_ref, q_out, qrecv)
    from_everyone(ndp, nt, lambda a, b: kv_out.at[a, b], kvrecv, ssem.at[0])
    swap_dp_finish(sends, ndp, q_out, qrecv)
    kv_own.wait()
    q_own.wait()
    sends.finish()


def gather_kernel(ndp, nt, a_ref, a_out, local, ssem, recv):
    dp, tn = where_am_i()
    meet(ndp, nt)
    sends = Sends(ssem)
    own = pltpu.make_async_copy(a_ref, a_out.at[dp], local.at[0])
    own.start()
    gather_start(sends, ndp, a_ref, a_out, recv)
    gather_finish(sends, ndp, a_out, recv)
    own.wait()
    sends.finish()


def swap_kernel(ndp, nt, a_ref, a_out, local, ssem, recv):
    dp, tn = where_am_i()
    meet(ndp, nt)
    sends = Sends(ssem)
    own = pltpu.make_async_copy(a_ref.at[dp], a_out.at[dp], local.at[0])
    own.start()
    swap_dp(sends, ndp, a_ref, a_out, recv)
    swap_dp_finish(sends, ndp, a_out, recv)
    own.wait()
    sends.finish()


def backward_kernel(ndp, nt, q_ref, kv_ref, q_out, kv_out, local, ssem, qrecv, kvrecv):
    dp, tn = where_am_i()
    meet(ndp, nt)
    sends = Sends(ssem)
    kv_own = pltpu.make_async_copy(kv_ref.at[tn], kv_out.at[dp, tn], local.at[0])
    q_own = pltpu.make_async_copy(q_ref, q_out.at[dp], local.at[1])
    kv_own.start()
    q_own.start()
    to_everyone(sends, ndp, nt, lambda a, b: kv_ref.at[b], kv_out.at[dp, tn], kvrecv)
    gather_start(sends, ndp, q_ref, q_out, qrecv)
    gather_finish(sends, ndp, q_out, qrecv)
    from_everyone(ndp, nt, lambda a, b: kv_out.at[a, b], kvrecv, ssem.at[0])
    kv_own.wait()
    q_own.wait()
    sends.finish()


def tensor_swap_kernel(ndp, nt, a_ref, a_out, local, ssem, recv):
    dp, tn = where_am_i()
    meet(ndp, nt)
    sends = Sends(ssem)
    own = pltpu.make_async_copy(a_ref.at[tn], a_out.at[tn], local.at[0])
    own.start()
    for k in range(1, nt):
        other = lax.rem(tn + k, nt)
        sends.go(a_ref.at[other], a_out.at[tn], recv.at[tn], dp, other)
    for k in range(1, nt):
        other = lax.rem(tn + nt - k, nt)
        copy_to(a_out.at[other], a_out.at[other], ssem.at[0], recv.at[other], dp, other).wait_recv()
    own.wait()
    sends.finish()


def home_kernel(ndp, nt, a_ref, a_out, local, ssem, recv):
    dp, tn = where_am_i()
    per = ndp // nt
    meet(ndp, nt)
    started = []
    for m in range(per):
        target, owner = m * nt + tn, dp // per
        slot = lax.rem(dp, per)
        mine = jnp.logical_and(target == dp, owner == tn)
        copy = copy_to(a_ref.at[m], a_out.at[slot], ssem.at[m], recv.at[slot], target, owner)
        here = pltpu.make_async_copy(a_ref.at[m], a_out.at[slot], local.at[0])

        @pl.when(mine)
        def _():
            here.start()
            here.wait()

        @pl.when(jnp.logical_not(mine))
        def _():
            copy.start()

        started.append((mine, copy))
    for s in range(per):
        source, relay = tn * per + s, lax.rem(dp, nt)
        mine = jnp.logical_and(source == dp, relay == tn)

        @pl.when(jnp.logical_not(mine))
        def _():
            copy_to(a_out.at[s], a_out.at[s], ssem.at[0], recv.at[s], source, relay).wait_recv()

    for mine, copy in started:

        @pl.when(jnp.logical_not(mine))
        def _():
            copy.wait_send()


def last_kernel(ndp, nt, r_ref, g_ref, r_out, g_out, local, ssem, rrecv, grecv):
    dp, tn = where_am_i()
    meet(ndp, nt)
    sends = Sends(ssem)
    r_own = pltpu.make_async_copy(r_ref, r_out.at[tn], local.at[0])
    g_own = pltpu.make_async_copy(g_ref, g_out.at[dp], local.at[1])
    r_own.start()
    g_own.start()
    for k in range(1, nt):
        sends.go(r_ref, r_out.at[tn], rrecv.at[tn], dp, lax.rem(tn + k, nt))
    for k in range(1, ndp):
        sends.go(g_ref, g_out.at[dp], grecv.at[dp], lax.rem(dp + k, ndp), tn)
    for k in range(1, nt):
        other = lax.rem(tn + nt - k, nt)
        copy_to(r_out.at[other], r_out.at[other], ssem.at[0], rrecv.at[other], dp, other).wait_recv()
    swap_dp_finish(sends, ndp, g_out, grecv)
    r_own.wait()
    g_own.wait()
    sends.finish()


def send(kernel, number, ndp, nt, arrays, shapes, sends, recvs):
    dma = pltpu.SemaphoreType.DMA
    many = len(shapes) > 1
    outs = [jax.ShapeDtypeStruct(shape, array.dtype) for shape, array in zip(shapes, arrays)]
    specs = [pl.BlockSpec(memory_space=VMEM)] * len(arrays)
    return pl.pallas_call(
        functools.partial(kernel, ndp, nt),
        out_shape=outs if many else outs[0],
        in_specs=specs,
        out_specs=specs if many else specs[0],
        scratch_shapes=[dma((2,)), dma((sends,))] + [dma((count,)) for count in recvs],
        compiler_params=pltpu.CompilerParams(collective_id=number, has_side_effects=True),
        name=kernel.__name__,
    )(*arrays)


def turn(field, cosine, sine, axis, back):
    front, rear = jnp.split(field, 2, axis)
    sine = -sine if back else sine
    return jnp.concatenate([front * cosine - rear * sine, rear * cosine + front * sine], axis)


def on_device(ndp, nt, checkpoint, norm_gain, w_query, w_key, w_value, grad_attn):
    rows, own_width = checkpoint.shape
    features, q_width = w_query.shape
    k_width = w_key.shape[1]
    entries = k_width // KVHEADS
    width = own_width * nt
    per = ndp // nt
    heads = q_width // HD
    seq = ndp * rows
    everyone = ndp * nt
    f32, bf16 = jnp.float32, jnp.bfloat16
    assert ndp == per * nt and nt % KVHEADS == 0 and heads * nt == QHEADS and features * per == own_width

    x_own = checkpoint.astype(f32)
    squares = jnp.sum(x_own * x_own, -1)
    gain_rows = jnp.broadcast_to(norm_gain.reshape(per, 1, features), (per, PAD, features))
    slices = jnp.concatenate(
        [jnp.transpose(checkpoint.reshape(rows, per, features), (1, 0, 2)), gain_rows], 1
    )
    x_all, squares_all = send(
        spread_kernel,
        1,
        ndp,
        nt,
        (slices, jnp.broadcast_to(squares, (8, rows))),
        ((ndp, rows + PAD, features), (ndp, nt, 8, rows)),
        everyone + 4 * ndp,
        (ndp, everyone),
    )
    inverse_all = lax.rsqrt(jnp.sum(squares_all[:, :, 0], 1) / width + EPS)
    gain = x_all[0, rows].astype(f32)
    normed = (x_all[:, :rows].astype(f32) * inverse_all[:, :, None] * gain).astype(bf16)
    normed = normed.reshape(seq, features)

    q_terms = jnp.dot(normed, w_query, preferred_element_type=f32).astype(bf16)

    def entry_terms(matrix):
        terms = lax.dot_general(matrix, normed, (((0,), (1,)), ((), ())), preferred_element_type=f32)
        return terms.astype(bf16).reshape(entries, KVHEADS, ndp, rows)

    kv_terms = jnp.stack([entry_terms(w_key), entry_terms(w_value)])
    kv_terms = jnp.transpose(kv_terms, (2, 3, 0, 1, 4)).reshape(KVHEADS, ndp, 2 * entries, rows)
    q_parts, kv_parts = send(
        forward_kernel,
        2,
        ndp,
        nt,
        (q_terms.reshape(ndp, rows, q_width), kv_terms),
        ((ndp, rows, q_width), (ndp, nt, 2 * entries, rows)),
        everyone + ndp,
        (ndp, everyone),
    )
    dp = lax.axis_index("dp")
    positions = dp * rows + jnp.arange(rows, dtype=jnp.int32)
    frequency = THETA ** (-(jnp.arange(HD // 2, dtype=f32) * 2.0) / HD)
    angle = positions.astype(f32)[:, None] * frequency[None, :]
    cosine, sine = jnp.cos(angle), jnp.sin(angle)
    cosine_t, sine_t = cosine.T, sine.T
    queries = jnp.sum(q_parts.astype(f32), 0).reshape(rows, heads, HD)
    query_rot = turn(queries, cosine[:, None], sine[:, None], -1, False).astype(bf16)
    kv_sum = jnp.sum(kv_parts.astype(f32), 0).reshape(nt, 2, entries, rows)
    kv_sum = jnp.transpose(kv_sum, (1, 0, 2, 3)).reshape(2, HD, rows)
    key_rot = turn(kv_sum[0], cosine_t, sine_t, 0, False)
    kv_own = jnp.concatenate([key_rot, kv_sum[1]], 0).astype(bf16)
    kv_all = send(
        gather_kernel, 3, ndp, nt, (kv_own,), ((ndp, 2 * HD, rows),), 2 * ndp, (ndp,)
    )
    kv_all = jnp.transpose(kv_all, (1, 0, 2)).reshape(2, HD, seq)
    keys, values = kv_all[0], kv_all[1]

    score_scale = HD ** (-0.5)
    upstream = grad_attn.reshape(rows, heads, HD)
    scores = jnp.einsum("tgd,ds->gts", query_rot, keys, preferred_element_type=f32) * score_scale
    allowed = positions[:, None] >= jnp.arange(seq, dtype=jnp.int32)[None, :]
    scores = jnp.where(allowed, scores, -jnp.inf)
    raw = jnp.exp(scores - jnp.max(scores, -1, keepdims=True))
    chances = raw / jnp.sum(raw, -1, keepdims=True)
    chances_half = chances.astype(bf16)
    attended = jnp.einsum("gts,ds->tgd", chances_half, values, preferred_element_type=f32)
    row_delta = jnp.sum(upstream.astype(f32) * attended, -1)
    prob_grads = jnp.einsum("tgd,ds->gts", upstream, values, preferred_element_type=f32)
    dscore = (chances * (prob_grads - row_delta.T[..., None])).astype(bf16)
    dquery = jnp.einsum("gts,ds->tgd", dscore, keys, preferred_element_type=f32) * score_scale
    dkey = jnp.einsum("gts,tgd->ds", dscore, query_rot, preferred_element_type=f32) * score_scale
    dvalue = jnp.einsum("gts,tgd->ds", chances_half, upstream, preferred_element_type=f32)
    dkv = jnp.concatenate([dkey, dvalue], 0).astype(bf16).reshape(2 * HD, ndp, rows)
    dkv_parts = send(
        swap_kernel,
        4,
        ndp,
        nt,
        (jnp.transpose(dkv, (1, 0, 2)),),
        ((ndp, 2 * HD, rows),),
        ndp,
        (ndp,),
    )
    dkv_sum = jnp.sum(dkv_parts.astype(f32), 0)
    dkv_own = jnp.stack([turn(dkv_sum[:HD], cosine_t, sine_t, 0, True), dkv_sum[HD:]])
    dkv_own = dkv_own.astype(bf16).reshape(2, nt, entries, rows)
    dkv_own = jnp.transpose(dkv_own, (1, 0, 2, 3)).reshape(nt, 2 * entries, rows)
    dquery_pre = turn(dquery, cosine[:, None], sine[:, None], -1, True).astype(bf16)
    dq_all, dkv_all = send(
        backward_kernel,
        5,
        ndp,
        nt,
        (dquery_pre.reshape(rows, q_width), dkv_own),
        ((ndp, rows, q_width), (ndp, nt, 2 * entries, rows)),
        everyone + 2 * ndp,
        (ndp, everyone),
    )
    dq_all = dq_all.reshape(seq, q_width)
    dkv_all = dkv_all.reshape(ndp, KVHEADS, nt // KVHEADS, 2, entries, rows)
    dkv_all = jnp.sum(dkv_all.astype(f32), 2).astype(bf16)
    dkv_all = jnp.transpose(dkv_all, (2, 3, 1, 0, 4)).reshape(2, k_width, seq)

    def cols_back(matrix, grads):
        return lax.dot_general(grads, matrix, (((0,), (1,)), ((), ())), preferred_element_type=f32)

    partial = lax.dot_general(dq_all, w_query, (((1,), (1,)), ((), ())), preferred_element_type=f32)
    partial = partial + cols_back(w_key, dkv_all[0]) + cols_back(w_value, dkv_all[1])
    partial = partial.astype(bf16).reshape(per, nt, rows, features)
    swapped = send(
        tensor_swap_kernel,
        6,
        ndp,
        nt,
        (jnp.transpose(partial, (1, 0, 2, 3)),),
        ((nt, per, rows, features),),
        nt,
        (nt,),
    )
    summed = jnp.sum(swapped.astype(f32), 0).astype(bf16)
    homed = send(home_kernel, 7, ndp, nt, (summed,), ((per, rows, features),), per, (per,))
    dnormed = jnp.transpose(homed, (1, 0, 2)).reshape(rows, own_width).astype(f32)
    gain_own = norm_gain.astype(f32)
    inverse = lax.dynamic_index_in_dim(inverse_all, dp, 0, False)[:, None]
    row_part = jnp.sum(gain_own * dnormed * x_own, -1)
    gain_part = jnp.sum(dnormed * x_own * inverse, 0).reshape(-1, 128)
    row_parts, gain_parts = send(
        last_kernel,
        8,
        ndp,
        nt,
        (jnp.broadcast_to(row_part, (8, rows)), gain_part),
        ((nt, 8, rows), (ndp,) + gain_part.shape),
        ndp + nt,
        (nt, ndp),
    )
    row_sum = jnp.sum(row_parts[:, 0], 0)[:, None]
    d_checkpoint = (
        inverse * gain_own * dnormed - x_own * inverse**3 * row_sum / width
    ).astype(bf16)
    grad_gain = jnp.sum(gain_parts, 0).reshape(own_width)

    def weight_grad(grads, axis):
        return lax.dot_general(
            normed, grads, (((0,), (axis,)), ((), ())), preferred_element_type=f32
        )

    grad_query = weight_grad(dq_all, 0)
    grad_key = weight_grad(dkv_all[0], 1)
    grad_value = weight_grad(dkv_all[1], 1)
    return (d_checkpoint, grad_gain, grad_query, grad_key, grad_value)


def solution(mesh):
    tokens = P(("sweep", "dp"), "tensor")
    gains = P(("sweep", "tensor"))
    return jax.shard_map(
        functools.partial(on_device, mesh.shape["dp"], mesh.shape["tensor"]),
        mesh=mesh,
        in_specs=(tokens, gains, tokens, tokens, tokens, tokens),
        out_specs=(tokens, gains, tokens, tokens, tokens),
        check_vma=False,
    )
```
